32 devices in a mesh: dp: 16 (over z, x, core), tensor: 2 (over y).
Axes of the slice: x: 2, y: 2, z: 4, core: 2. Of those that a mesh axis runs over, the one named last changes fastest.
Arguments:
- activations: bfloat16 [4096, 2880], P(('dp', 'tensor')), parts along dimension 0, may hold values from -6 to 6
- segment_ids: int32 [4096], P('dp'), parts along dimension 0, may hold values from 0 to 3, as said below
- attn_gain: float32 [2880], replicated, may hold values from 0.1 to 1.9
- qkv_weight: bfloat16 [2880, 5120], P(None, 'tensor'), may hold values from -2 to 2
- out_weight: bfloat16 [4096, 2880], P('tensor'), may hold values from -0.09375 to 0.09375
- ffn_gain: float32 [2880], replicated, may hold values from 0.1 to 1.9
- gate_weight: bfloat16 [2880, 2048], P(None, 'tensor'), may hold values from -0.109375 to 0.109375
- up_weight: bfloat16 [2880, 2048], P(None, 'tensor'), may hold values from -0.109375 to 0.109375
- down_weight: bfloat16 [2048, 2880], P('tensor'), may hold values from -0.125 to 0.125
Outputs:
- layer_out: bfloat16 [4096, 2880], P(('dp', 'tensor')), parts along dimension 0
The draws below stay inside these ranges and needn't reach their ends.
There are 16 independent parts, one for each index of `dp`. The reference program is written for one: setup_inputs(seed, part) draws one part's arguments, and reference() takes and returns one part's arrays. A program takes and returns all parts, laid end to end along the dimension named above; an argument that names none is the same for every part. Nothing has to cross between parts.
Inputs may be any that keep to these rules, and one draw needn't show every extreme that they name: `segment_ids`: segment numbers never fall along the tokens, and each of the four segments holds at least one token.
All inputs are finite; a program needn't handle non-finite values.
Results may differ from the reference program's by a relative error of at most 0.035.
Values may be sent and summed in bfloat16 or wider, within the bound.
No kernel may reach another device: no remote copies, remote signals or barrier semaphores. Data moves between devices by JAX's collectives and lax.ppermute only.
A program may use at most 128 MiB of HBM per device.

```python
import jax
import jax.numpy as jnp
from jax import lax

D = 2880
HEADS = 64
KV_HEADS = 8
HEAD_DIM = 64
FF = 2048
TOKENS = 256
N_TENSOR = 2


def draw_segment_ids(key, part):
    cut_key = jax.random.fold_in(key, 7103)
    cuts = jax.random.permutation(cut_key, TOKENS - 1)[:3].astype(jnp.int32) + 1
    positions = jnp.arange(TOKENS, dtype=jnp.int32)
    above = (positions[:, None] >= cuts[None, :]).astype(jnp.int32)
    return jnp.sum(above, axis=1).astype(jnp.int32)


def draw_qkv_weight(key, part):
    width = (HEADS // KV_HEADS + 2) * HEAD_DIM
    first_key = jax.random.fold_in(key, 0)
    base = jnp.clip(jax.random.normal(first_key, (D, KV_HEADS, width), jnp.float32), -6.0, 6.0) * D ** (-0.5)
    return base.reshape(D, KV_HEADS * width).astype(jnp.bfloat16)


def block_levels(rng, shape, shards, smallest, top_value):
    def one(axis_at, blocks):
        heights = jax.random.uniform(jax.random.fold_in(jax.random.fold_in(rng, 6), axis_at), (blocks,), jnp.float32, smallest / len(shards), top_value / len(shards))
        return jnp.repeat(jnp.exp(heights), shape[axis_at] // blocks).reshape((-1,) + (1,) * (len(shape) - axis_at - 1))

    factor_of = one(*shards[0])
    for cut in shards[1:]:
        factor_of = factor_of * one(*cut)
    return factor_of


def normal_values(rng, dims, spread, bound, cuts=(), kind=jnp.bfloat16):
    values = jax.random.normal(rng, dims, jnp.float32) * spread
    if len(cuts) > 0:
        values = block_levels(rng, dims, cuts, -0.22, 0.18) * values
    return jnp.clip(values, min=-bound, max=bound).astype(kind)


def setup_inputs(seed: int = 0, part: int = 0) -> dict:
    streams_of = jax.random.split(jax.random.key(seed), 10)
    part_splits = jax.random.split(jax.random.fold_in(streams_of[9], part), 10)
    return {
        "activations": normal_values(part_splits[0], (TOKENS, D), 1.0, 6.0, ((0, 2),)),
        "segment_ids": draw_segment_ids(jax.random.fold_in(jax.random.fold_in(streams_of[9], part), 71), part),
        "attn_gain": jnp.clip(1.0 + 0.18 * jax.random.normal(streams_of[2], (D,), jnp.float32), 0.1, 1.9),
        "qkv_weight": draw_qkv_weight(jax.random.fold_in(streams_of[9], 71), part),
        "out_weight": normal_values(streams_of[4], (HEADS * HEAD_DIM, D), (HEADS * HEAD_DIM) ** -0.5, 0.09375, ((0, 2),)),
        "ffn_gain": jnp.clip(1.0 + 0.18 * jax.random.normal(streams_of[5], (D,), jnp.float32), 0.1, 1.9),
        "gate_weight": normal_values(streams_of[6], (D, FF), D ** -0.5, 0.109375, ((1, 2),)),
        "up_weight": normal_values(streams_of[7], (D, FF), D ** -0.5, 0.109375, ((1, 2),)),
        "down_weight": normal_values(streams_of[8], (FF, D), FF ** -0.5, 0.125, ((0, 2),)),
    }


def normalize(rows_in, gain):
    floats = rows_in.astype(jnp.float32)
    mean_square = lax.optimization_barrier(jnp.mean(floats * floats, axis=-1, keepdims=True))
    return (floats * lax.rsqrt(mean_square + 1e-05) * gain).astype(jnp.bfloat16)

def grouped_sum(left, right):
    group_rows = right.shape[0] // N_TENSOR
    total = jnp.zeros((left.shape[0], right.shape[1]), jnp.float32)
    for group in range(N_TENSOR):
        part_left = left[:, group * group_rows:(group + 1) * group_rows]
        part_right = right[group * group_rows:(group + 1) * group_rows]
        partial_out = jnp.dot(part_left, part_right, preferred_element_type=jnp.float32).astype(jnp.bfloat16)
        total = total + partial_out.astype(jnp.float32)
    return total

def reference(activations, segment_ids, attn_gain, qkv_weight, out_weight, ffn_gain, gate_weight, up_weight, down_weight):
    group_size = HEADS // KV_HEADS
    normed = normalize(activations, attn_gain)
    projected = jnp.dot(normed, qkv_weight, preferred_element_type=jnp.float32).astype(jnp.bfloat16)
    projected = projected.reshape(TOKENS, KV_HEADS, group_size + 2, HEAD_DIM)
    queries = projected[:, :, :group_size].astype(jnp.float32)
    key_rows = projected[:, :, group_size].astype(jnp.float32)
    value_rows = projected[:, :, group_size + 1].astype(jnp.float32)
    scores = jnp.einsum('sngd,tnd->ngst', queries, key_rows) * HEAD_DIM ** (-0.5)
    positions = jnp.arange(TOKENS, dtype=jnp.int32)
    allowed = (positions[None, :] <= positions[:, None]) & (segment_ids[None, :] == segment_ids[:, None])
    scores = jnp.where(allowed, scores, -1e+30)
    row_max = lax.optimization_barrier(jnp.max(scores, axis=-1, keepdims=True))
    weights = jnp.exp(scores - row_max)
    row_total = lax.optimization_barrier(jnp.sum(weights, axis=-1, keepdims=True))
    softmax_out = lax.optimization_barrier((weights / row_total).astype(jnp.bfloat16))
    mixed = jnp.einsum('ngst,tnd->sngd', softmax_out.astype(jnp.float32), value_rows)
    mixed_heads = mixed.astype(jnp.bfloat16).reshape(TOKENS, HEADS * HEAD_DIM)
    attn_proj = grouped_sum(mixed_heads, out_weight)
    resid_sum = (activations.astype(jnp.float32) + attn_proj).astype(jnp.bfloat16)
    ffn_input = normalize(resid_sum, ffn_gain)
    gate_act = jnp.dot(ffn_input, gate_weight, preferred_element_type=jnp.float32)
    up_act = jnp.dot(ffn_input, up_weight, preferred_element_type=jnp.float32)
    hidden = (jax.nn.silu(gate_act) * up_act).astype(jnp.bfloat16)
    ffn_out = grouped_sum(hidden, down_weight)
    return (resid_sum.astype(jnp.float32) + ffn_out).astype(jnp.bfloat16)
```

```python
import functools

import jax
import jax.numpy as jnp
from jax import lax
from jax.experimental import pallas as pl
from jax.experimental.pallas import tpu as pltpu
from jax.sharding import PartitionSpec as P

HEADS = 64
KV_HEADS = 8
HEAD_DIM = 64
PARTS = 4
STEPS = 3
FEED_STEPS = 4


def normalize(rows_in, gain):
    floats = rows_in.astype(jnp.float32)
    mean_square = jnp.mean(floats * floats, axis=-1, keepdims=True)
    return (floats * lax.rsqrt(mean_square + 1e-05) * gain).astype(jnp.bfloat16)


def attend(projected, segment_ids):
    token_count = projected.shape[0]
    group_size = HEADS // KV_HEADS
    heads_view = projected.reshape(token_count, -1, group_size + 2, HEAD_DIM)
    key_rows = heads_view[:, :, group_size]
    value_rows = heads_view[:, :, group_size + 1]
    block_rows = token_count if token_count <= 512 else 512
    block_count = token_count // block_rows
    positions = jnp.arange(token_count, dtype=jnp.int32)

    def one_block(block_index):
        first_row = block_index * block_rows
        query_rows = lax.dynamic_slice_in_dim(heads_view, first_row, block_rows, 0)[
            :, :, :group_size
        ]
        query_pos = first_row + jnp.arange(block_rows, dtype=jnp.int32)
        query_seg = lax.dynamic_slice_in_dim(segment_ids, first_row, block_rows, 0)
        scores = jnp.einsum(
            "sngd,tnd->ngst", query_rows, key_rows, preferred_element_type=jnp.float32
        ) * HEAD_DIM ** (-0.5)
        allowed = (positions[None, :] <= query_pos[:, None]) & (
            segment_ids[None, :] == query_seg[:, None]
        )
        scores = jnp.where(allowed, scores, -1e30)
        row_max = jnp.max(scores, axis=-1, keepdims=True)
        weights = jnp.exp(scores - row_max)
        row_total = jnp.sum(weights, axis=-1, keepdims=True)
        softmax_out = (weights / row_total).astype(jnp.bfloat16)
        mixed = jnp.einsum(
            "ngst,tnd->sngd", softmax_out, value_rows, preferred_element_type=jnp.float32
        )
        return mixed.astype(jnp.bfloat16)

    blocks_out = lax.map(one_block, jnp.arange(block_count, dtype=jnp.int32))
    return blocks_out.reshape(token_count, -1)


def shards(
    activations,
    segment_ids,
    attn_gain,
    qkv_weight,
    out_weight,
    ffn_gain,
    gate_weight,
    up_weight,
    down_weight,
):
    own_rows = activations.shape[0]
    whole_rows = lax.all_gather(activations, "tensor", axis=0, tiled=True)
    projected = jnp.dot(
        normalize(whole_rows, attn_gain), qkv_weight, preferred_element_type=jnp.float32
    ).astype(jnp.bfloat16)
    mixed_heads = attend(projected, segment_ids)
    head_total = lax.psum(
        jnp.dot(mixed_heads, out_weight, preferred_element_type=jnp.float32).astype(jnp.bfloat16),
        "tensor",
    ).astype(jnp.float32)
    resid_whole = (whole_rows.astype(jnp.float32) + head_total).astype(jnp.bfloat16)
    shard_rows = normalize(resid_whole, ffn_gain)
    gate_act = jnp.dot(shard_rows, gate_weight, preferred_element_type=jnp.float32)
    up_act = jnp.dot(shard_rows, up_weight, preferred_element_type=jnp.float32)
    hidden = (jax.nn.silu(gate_act) * up_act).astype(jnp.bfloat16)
    resid_sum = lax.dynamic_slice_in_dim(
        resid_whole, lax.axis_index("tensor") * own_rows, own_rows, 0
    )
    ffn_out = lax.psum_scatter(
        jnp.dot(hidden, down_weight, preferred_element_type=jnp.float32).astype(jnp.bfloat16),
        "tensor",
        scatter_dimension=0,
        tiled=True,
    ).astype(jnp.float32)
    return (resid_sum.astype(jnp.float32) + ffn_out).astype(jnp.bfloat16)


def turn(block):
    return block.astype(jnp.float32).T


def row_scale(floats):
    mean_square = jnp.sum(floats * floats, axis=0, keepdims=True) * (1.0 / floats.shape[0])
    return lax.rsqrt(mean_square + 1e-05)


def hbm():
    return pl.BlockSpec(memory_space=pl.ANY)


def params(mib, steps=0):
    return pltpu.CompilerParams(
        vmem_limit_bytes=mib * 2**20, dimension_semantics=("arbitrary",) * steps if steps else None
    )


def project_own_kernel(x_ref, gain_ref, weight_ref, out_ref, rows_ref, scale_ref):
    @pl.when(pl.program_id(0) == 0)
    def _():
        floats = x_ref[...].astype(jnp.float32)
        scale_ref[...] = jnp.broadcast_to(row_scale(floats), scale_ref.shape)
        rows_ref[...] = (floats.T * gain_ref[...]).astype(jnp.bfloat16)

    product = jnp.dot(rows_ref[...], weight_ref[...], preferred_element_type=jnp.float32)
    out_ref[...] = (product.T * scale_ref[:1]).astype(jnp.bfloat16)


def project_own(x_t, gain, weight, name):
    dim, tokens = x_t.shape
    columns = weight.shape[1]
    block = (HEADS // KV_HEADS + 2) * HEAD_DIM
    return pl.pallas_call(
        project_own_kernel,
        name=name,
        grid=(columns // block,),
        in_specs=[
            pl.BlockSpec((dim, tokens), lambda i: (0, 0)),
            pl.BlockSpec((1, dim), lambda i: (0, 0)),
            pl.BlockSpec((dim, block), lambda i: (0, i)),
        ],
        out_specs=pl.BlockSpec((block, tokens), lambda i: (i, 0)),
        out_shape=jax.ShapeDtypeStruct((columns, tokens), jnp.bfloat16),
        scratch_shapes=[
            pltpu.VMEM((tokens, dim), jnp.bfloat16),
            pltpu.VMEM((8, tokens), jnp.float32),
        ],
        compiler_params=params(40, 1),
    )(x_t, gain, weight)


def attend_group(queries_t, keys_t, values_t, bias):
    heads = queries_t.shape[0] // HEAD_DIM
    tokens = queries_t.shape[1]
    side = jnp.concatenate(
        [queries_t[h * HEAD_DIM:(h + 1) * HEAD_DIM] for h in range(heads)], axis=1
    )
    key_rows = turn(keys_t).astype(jnp.bfloat16)
    scores = jnp.dot(key_rows, side, preferred_element_type=jnp.float32)
    probs = []
    for h in range(heads):
        part = scores[:, h * tokens:(h + 1) * tokens] + bias
        weights = jnp.exp(part - jnp.max(part, axis=0, keepdims=True))
        inverse = 1.0 / jnp.sum(weights, axis=0, keepdims=True)
        probs.append((weights * inverse).astype(jnp.bfloat16))
    mixed = jnp.dot(values_t, jnp.concatenate(probs, axis=1), preferred_element_type=jnp.float32)
    mixed = mixed.astype(jnp.bfloat16)
    return jnp.concatenate([mixed[:, h * tokens:(h + 1) * tokens] for h in range(heads)], axis=0)


def attend_own_kernel(count, width, *refs):
    x_refs = refs[:count]
    (gain_ref, own_ref, bias_ref, weight_ref, out_weight_ref) = refs[count:count + 5]
    (rows_ref, scale_ref, kv_ref, mixed_ref, first_ref) = refs[count + 5:count + 10]
    (weights, out_weights, sems, out_sem) = refs[count + 10:]
    groups = own_ref.shape[0] // width
    group_rows = width - 2 * HEAD_DIM

    def fetch(g):
        return pltpu.make_async_copy(
            weight_ref.at[:, pl.ds(g * width + group_rows, 2 * HEAD_DIM)], weights.at[g], sems.at[g]
        )

    out_copy = pltpu.make_async_copy(
        out_weight_ref.at[pl.ds(0, out_weights.shape[0])], out_weights, out_sem
    )
    for g in range(groups):
        fetch(g).start()
    out_copy.start()
    at = 0
    total = 0.0
    for x_ref in x_refs:
        floats = x_ref[...].astype(jnp.float32)
        total = total + jnp.sum(floats * floats, axis=0, keepdims=True)
        size = x_ref.shape[0]
        rows_ref[:, at:at + size] = (floats.T * gain_ref[:, at:at + size]).astype(jnp.bfloat16)
        at += size
    scale = lax.rsqrt(total * (1.0 / at) + 1e-05)
    scale_ref[...] = jnp.broadcast_to(scale, scale_ref.shape)
    for g in range(groups):
        fetch(g).wait()
        product = jnp.dot(rows_ref[...], weights[g], preferred_element_type=jnp.float32)
        kv_ref[g * 2 * HEAD_DIM:(g + 1) * 2 * HEAD_DIM] = (product.T * scale).astype(jnp.bfloat16)

    def one_group(g, carry):
        start = pl.multiple_of(g * width, HEAD_DIM)
        kv_start = pl.multiple_of(g * 2 * HEAD_DIM, HEAD_DIM)
        queries_t = own_ref[pl.ds(start, group_rows)] * HEAD_DIM**-0.5
        own_kv = own_ref[pl.ds(pl.multiple_of(start + group_rows, HEAD_DIM), 2 * HEAD_DIM)]
        peer_kv = kv_ref[pl.ds(kv_start, 2 * HEAD_DIM)]
        both = jnp.concatenate([own_kv, peer_kv], axis=1)
        mixed_ref[pl.ds(pl.multiple_of(g * group_rows, HEAD_DIM), group_rows)] = attend_group(
            queries_t, both[:HEAD_DIM], both[HEAD_DIM:], bias_ref[...]
        )
        return carry

    lax.fori_loop(0, groups, one_group, 0)
    out_copy.wait()
    first_ref[...] = jnp.dot(
        out_weights[...], mixed_ref[...], preferred_element_type=jnp.float32
    ).astype(jnp.bfloat16)


def attend_own(x_parts, gain, own_t, bias, weight, out_weight_t, size, name):
    dim, columns = weight.shape
    tokens = own_t.shape[1]
    width = (HEADS // KV_HEADS + 2) * HEAD_DIM
    groups = columns // width
    count = len(x_parts)
    vmem = pl.BlockSpec(memory_space=pltpu.VMEM)
    mixed_rows = groups * (width - 2 * HEAD_DIM)
    return pl.pallas_call(
        functools.partial(attend_own_kernel, count, width),
        name=name,
        in_specs=[vmem] * (count + 3) + [hbm(), hbm()],
        out_specs=[vmem] * 5,
        out_shape=[
            jax.ShapeDtypeStruct((tokens, dim), jnp.bfloat16),
            jax.ShapeDtypeStruct((8, tokens), jnp.float32),
            jax.ShapeDtypeStruct((groups * 2 * HEAD_DIM, tokens), jnp.bfloat16),
            jax.ShapeDtypeStruct((mixed_rows, tokens), jnp.bfloat16),
            jax.ShapeDtypeStruct((size, tokens), jnp.bfloat16),
        ],
        scratch_shapes=[
            pltpu.VMEM((groups, dim, 2 * HEAD_DIM), jnp.bfloat16),
            pltpu.VMEM((size, mixed_rows), jnp.bfloat16),
            pltpu.SemaphoreType.DMA((groups,)),
            pltpu.SemaphoreType.DMA,
        ],
        compiler_params=params(40),
    )(*x_parts, gain, own_t, bias, weight, out_weight_t)


def attend_peer_kernel(rows_ref, scale_ref, own_kv_ref, kv_ref, bias_ref, weight_ref, mixed_ref):
    group_rows = weight_ref.shape[1] - 2 * HEAD_DIM
    product = jnp.dot(
        rows_ref[...], weight_ref[:, :group_rows], preferred_element_type=jnp.float32
    )
    queries_t = (product.T * scale_ref[:1]).astype(jnp.bfloat16) * HEAD_DIM**-0.5
    both = jnp.concatenate([own_kv_ref[...], kv_ref[...]], axis=1)
    mixed_ref[...] = attend_group(queries_t, both[:HEAD_DIM], both[HEAD_DIM:], bias_ref[...])


def attend_peer(rows, scale, own_t, kv, bias, weight, name):
    dim, columns = weight.shape
    tokens = rows.shape[0]
    per_group = HEADS // KV_HEADS
    width = (per_group + 2) * HEAD_DIM
    groups = columns // width
    group_rows = per_group * HEAD_DIM
    kv_at = width // (2 * HEAD_DIM)
    return pl.pallas_call(
        attend_peer_kernel,
        name=name,
        grid=(groups,),
        in_specs=[
            pl.BlockSpec((tokens, dim), lambda g: (0, 0)),
            pl.BlockSpec((8, tokens), lambda g: (0, 0)),
            pl.BlockSpec((2 * HEAD_DIM, tokens), lambda g: ((g + 1) * kv_at - 1, 0)),
            pl.BlockSpec((2 * HEAD_DIM, tokens), lambda g: (g, 0)),
            pl.BlockSpec(bias.shape, lambda g: (0, 0)),
            pl.BlockSpec((dim, width), lambda g: (0, g)),
        ],
        out_specs=pl.BlockSpec((group_rows, tokens), lambda g: (g, 0)),
        out_shape=jax.ShapeDtypeStruct((groups * group_rows, tokens), jnp.bfloat16),
        compiler_params=params(40, 1),
    )(rows, scale, own_t, kv, bias, weight)


def project_out_kernel(mixed_ref, weight_ref, out_ref):
    out_ref[...] = jnp.dot(
        weight_ref[...], mixed_ref[...], preferred_element_type=jnp.float32
    ).astype(jnp.bfloat16)


def project_out(mixed_t, weight_t, first_row, size, name):
    depth, tokens = mixed_t.shape
    block = size // STEPS
    first_block = first_row // block
    return pl.pallas_call(
        project_out_kernel,
        name=name,
        grid=(STEPS,),
        in_specs=[
            pl.BlockSpec((depth, tokens), lambda i: (0, 0)),
            pl.BlockSpec((block, depth), lambda i: (first_block + i, 0)),
        ],
        out_specs=pl.BlockSpec((block, tokens), lambda i: (i, 0)),
        out_shape=jax.ShapeDtypeStruct((size, tokens), jnp.bfloat16),
        compiler_params=params(40, 1),
    )(mixed_t, weight_t)


def feed_kernel(count, steps, last, *refs):
    x_refs = refs[:count]
    mine_refs = refs[count:2 * count]
    came_refs = refs[2 * count:3 * count]
    gain_ref, gate_ref, up_ref, down_ref = refs[3 * count:3 * count + 4]
    outs = refs[3 * count + 4:-4]
    rows_ref, scale_ref, hidden_ref, resid_ref = refs[-4:]
    step = pl.program_id(0)

    @pl.when(step == 0)
    def _():
        at = 0
        total = 0.0
        for x_ref, mine_ref, came_ref in zip(x_refs, mine_refs, came_refs):
            size = x_ref.shape[0]
            both = mine_ref[...].astype(jnp.float32) + came_ref[...].astype(jnp.float32)
            resid = (x_ref[...].astype(jnp.float32) + both).astype(jnp.bfloat16)
            resid_ref[at:at + size] = resid
            floats = resid.astype(jnp.float32)
            total = total + jnp.sum(floats * floats, axis=0, keepdims=True)
            rows_ref[:, at:at + size] = (floats.T * gain_ref[:, at:at + size]).astype(jnp.bfloat16)
            at += size
        scale = lax.rsqrt(total * (1.0 / at) + 1e-05)
        scale_ref[...] = jnp.broadcast_to(scale, scale_ref.shape)

    @pl.when(step < steps)
    def _():
        rows = rows_ref[...]
        scale = scale_ref[:1]
        gate = jnp.dot(rows, gate_ref[...], preferred_element_type=jnp.float32).T * scale
        up = jnp.dot(rows, up_ref[...], preferred_element_type=jnp.float32).T * scale
        block = gate.shape[0]
        hidden_ref[pl.ds(pl.multiple_of(step * block, block), block)] = (
            gate / (1.0 + jnp.exp(-gate)) * up
        ).astype(jnp.bfloat16)

    for part in range(count):
        @pl.when(step == steps + part)
        def _(part=part):
            product = jnp.dot(
                down_ref[...], hidden_ref[...], preferred_element_type=jnp.float32
            ).astype(jnp.bfloat16)
            if last:
                size = product.shape[0]
                resid = resid_ref[part * size:(part + 1) * size].astype(jnp.float32)
                outs[part][...] = resid + product.astype(jnp.float32)
            else:
                outs[part][...] = product


def feed(x_parts, mine_parts, came_parts, gain, gate, up, down_t, last, name):
    count = len(x_parts)
    size, tokens = x_parts[0].shape
    dim, units = gate.shape
    steps = FEED_STEPS
    block = units // steps
    whole = pl.BlockSpec((size, tokens), lambda i: (0, 0))
    column = pl.BlockSpec((dim, block), lambda i: (0, jnp.minimum(i, steps - 1)))
    return pl.pallas_call(
        functools.partial(feed_kernel, count, steps, last),
        name=name,
        grid=(steps + count,),
        in_specs=[whole] * (3 * count) + [
            pl.BlockSpec((1, dim), lambda i: (0, 0)),
            column,
            column,
            pl.BlockSpec((size, units), lambda i: (jnp.maximum(i - steps, 0), 0)),
        ],
        out_specs=[whole] * count,
        out_shape=[
            jax.ShapeDtypeStruct((size, tokens), jnp.float32 if last else jnp.bfloat16)
        ] * count,
        scratch_shapes=[
            pltpu.VMEM((tokens, dim), jnp.bfloat16),
            pltpu.VMEM((8, tokens), jnp.float32),
            pltpu.VMEM((units, tokens), jnp.bfloat16),
            pltpu.VMEM((dim, tokens), jnp.bfloat16),
        ],
        compiler_params=params(40, 1),
    )(*x_parts, *mine_parts, *came_parts, gain, gate, up, down_t)


def finish_kernel(count, *refs):
    out_ref = refs[-1]
    size = refs[0].shape[0]
    for part in range(count):
        out_ref[part * size:(part + 1) * size] = (
            refs[part][...] + refs[count + part][...].astype(jnp.float32)
        ).astype(jnp.bfloat16)


def finish(base_parts, came_parts, name):
    count = len(base_parts)
    size, tokens = base_parts[0].shape
    vmem = pl.BlockSpec(memory_space=pltpu.VMEM)
    return pl.pallas_call(
        functools.partial(finish_kernel, count),
        name=name,
        in_specs=[vmem] * (2 * count),
        out_specs=vmem,
        out_shape=jax.ShapeDtypeStruct((count * size, tokens), jnp.bfloat16),
        compiler_params=params(40),
    )(*base_parts, *came_parts)


def pair_shards(
    activations,
    segment_ids,
    attn_gain,
    qkv_weight,
    out_weight,
    ffn_gain,
    gate_weight,
    up_weight,
    down_weight,
):
    tokens, dim = activations.shape
    size = dim // PARTS
    at = lax.axis_index("tensor")
    swap = lambda block: lax.ppermute(block, "tensor", [(0, 1), (1, 0)])
    x_t = activations.T
    out_weight_t = out_weight.T
    down_t = down_weight.T
    attn_gain = attn_gain.reshape(1, dim)
    ffn_gain = ffn_gain.reshape(1, dim)
    x_own = [x_t[i * size:(i + 1) * size] for i in range(PARTS)]
    x_peer = [swap(part) for part in x_own]

    segments = segment_ids.reshape(2, tokens)
    own_first = jnp.stack([segments[at], segments[1 - at]]).reshape(-1)
    offsets = jnp.stack([at, 1 - at]).astype(jnp.int32) * tokens
    positions = (offsets[:, None] + jnp.arange(tokens, dtype=jnp.int32)[None]).reshape(-1)
    allowed = (positions[:, None] <= positions[None, :]) & (
        own_first[:, None] == own_first[None, :]
    )
    bias = jnp.where(allowed, 0.0, -1e30).astype(jnp.float32)
    bias_own, bias_peer = bias[:, :tokens], bias[:, tokens:]

    own_t = project_own(x_t, attn_gain, qkv_weight, "project_own")
    rows, scale, kv, mixed, first = attend_own(
        x_peer, attn_gain, own_t, bias_own, qkv_weight, out_weight_t, size, "attend_own"
    )
    mine_own = [first] + [
        project_out(mixed, out_weight_t, i * size, size, f"out_own_{i}") for i in range(1, PARTS)
    ]
    came_peer = [swap(part) for part in mine_own]
    rows, _ = lax.optimization_barrier((rows, mine_own[-1]))
    mixed_peer = attend_peer(rows, scale, own_t, kv, bias_peer, qkv_weight, "attend_peer")
    mine_peer = [
        project_out(mixed_peer, out_weight_t, i * size, size, f"out_peer_{i}")
        for i in range(PARTS)
    ]
    came_own = [swap(part) for part in mine_peer]
    units_peer = feed(
        x_peer, mine_peer, came_peer, ffn_gain, gate_weight, up_weight, down_t, False, "feed_peer"
    )
    units_came = [swap(part) for part in units_peer]
    base = feed(
        x_own, mine_own, came_own, ffn_gain, gate_weight, up_weight, down_t, True, "feed_own"
    )
    return finish(base, units_came, "finish").T


def solution(mesh):
    placed = (
        P(("dp", "tensor"), None),
        P("dp"),
        P(),
        P(None, "tensor"),
        P("tensor", None),
        P(),
        P(None, "tensor"),
        P(None, "tensor"),
        P("tensor", None),
    )
    return jax.shard_map(
        pair_shards if mesh.shape["tensor"] == 2 else shards,
        mesh=mesh,
        in_specs=placed,
        out_specs=P(("dp", "tensor"), None),
        check_vma=False,
    )
```
